512 devices in a mesh: front: 128 (over y, x, z_lo, core), sub: 4 (over z_hi).
Axes of the slice: x: 4, y: 8, z: 8 (z_hi: 4, z_lo: 2; z = z_hi * 2 + z_lo), core: 2. Of those that a mesh axis runs over, the one named last changes fastest.
Arguments:
- row_values: float32 [65536, 1024], P(('front', 'sub')), may hold values from -0.12 to 0.12
- front_of_row: int32 [65536, 1], P(('front', 'sub')), may hold values from 0 to 127; in each aligned block of 128 rows (0 to 127, 128 to 255, ...) at most 2 rows name the same one
- child_factors: float32 [256, 512, 512], P('front', 'sub'), as said below
- child_columns: int32 [256, 512], P('front'), may hold values from 0 to 1023, as said below
- damping: float32 [128, 1024], P('front'), may hold values from 0.5 to 2
Outputs:
- front_factor: float32 [128, 1024, 1024], P('front', 'sub')
The draws below stay inside these ranges and needn't reach their ends.
Inputs may be any that keep to these rules, and one draw needn't show every extreme that they name: `front_of_row`: among the 128 rows of one device, at most 2 name the same front, and some device's block reaches this bound. `child_factors`: each block is upper triangular with a positive diagonal. `child_columns`: each row names 512 distinct columns.
All inputs are finite; a program needn't handle non-finite values.
Results may differ from the reference program's by a relative error of at most 0.0003.
Values sent between devices are 32-bit elements; how exact they have to be, the bound alone decides.
A program may use at most 64 MiB of HBM per device.

```python
import math
import jax
import jax.numpy as jnp
import numpy as np
from jax import lax

CONTRIB = 512
F = 1024
ROWS_SRC = 128
FRONTS = 128
MOST = 2
ROWS = 65536
N_FRONT = 128
N_SUB = 4


def draw_child_factors(key, part):
    key_diag = jax.random.fold_in(key, 11)
    key_off = jax.random.fold_in(key, 12)
    shape = (2 * FRONTS, CONTRIB, CONTRIB)
    diagonal = jnp.exp(jax.random.uniform(key_diag, (2 * FRONTS, CONTRIB), jnp.float32, jnp.log(0.5), jnp.log(2.0)))
    offdiag = jnp.clip(jax.random.normal(key_off, shape, jnp.float32), -5.0, 5.0) * (0.5 / jnp.sqrt(jnp.float32(CONTRIB)))
    upper_mask = jnp.triu(jnp.ones((CONTRIB, CONTRIB), jnp.float32), 1)
    eye_mask = jnp.eye(CONTRIB, dtype=jnp.float32)
    return (offdiag * upper_mask[None] + diagonal[:, :, None] * eye_mask[None]).astype(jnp.float32)


def draw_child_columns(key, part):
    key_score = jax.random.fold_in(key, 21)
    scores = jax.random.randint(key_score, (2 * FRONTS, F), 0, 2 ** 19, jnp.int32)
    distinct = scores * F + jnp.arange(F, dtype=jnp.int32)[None, :]
    permuted = jnp.argsort(distinct, axis=1, stable=True).astype(jnp.int32)
    return permuted[:, :CONTRIB]


def level_of(key, extent, cuts, low, largest):
    gain = 1.0
    for position, parts in cuts:
        steps = jax.random.uniform(jax.random.fold_in(jax.random.fold_in(key, 6), position), (parts,), jnp.float32, low / len(cuts), largest / len(cuts))
        gain = gain * jnp.repeat(jnp.exp(steps), extent[position] // parts).reshape((-1,) + (1,) * (len(extent) - 1 - position))
    return gain


def shared_out(stream_key, own, number, rows, number_of, top, reach, skew):
    order = jax.random.permutation(stream_key, number_of)
    crowded, usual = load_shares(number_of, rows * top, reach, skew, True), load_shares(number_of, rows * top, reach, skew, False)
    places = jnp.arange(number_of)

    def named(tallies, rotation):
        used = int((tallies > 0).sum())
        fixed = max(1, used // 4)
        passed = fixed + (places - fixed + rotation * (used - fixed)) % max(1, number_of - fixed)
        return jnp.zeros((number_of,), jnp.int32).at[order[jnp.where(places < fixed, places, passed)]].set(jnp.asarray(tallies, jnp.int32))

    tallies = jnp.where(number % 4 == 0, named(crowded, number // 4), named(usual, number - number // 4 - 1))
    mixed = jax.random.permutation(jax.random.fold_in(own, 3), number_of)
    giver, taker = mixed[0:number_of // 2 * 2:2], mixed[1:number_of // 2 * 2:2]
    slack = jnp.minimum(tallies[giver] - 1, reach - tallies[taker]) // 2
    slack = jnp.where((giver == order[0]) | (taker == order[0]) | (tallies[taker] == 0), 0, jnp.maximum(slack, 0))
    passed = jax.random.randint(jax.random.fold_in(own, 4), (number_of // 2,), 0, 1 << 20) % (slack + 1)
    tallies = tallies.at[giver].add(-passed).at[taker].add(passed)
    items = jnp.searchsorted(jnp.cumsum(tallies), jnp.arange(rows * top), side="right").astype(jnp.int32)
    listing = items.reshape(top, rows).T
    listing = listing[jax.random.permutation(jax.random.fold_in(own, 1), rows)]
    rotation = jax.random.randint(jax.random.fold_in(own, 2), (rows, 1), 0, top)
    return jnp.take_along_axis(listing, (jnp.arange(top)[None, :] + rotation) % top, axis=1)


def load_shares(number_of, total, limit, slope, full):
    portions = [(1 << 20) // math.isqrt(rank ** slope) + 1 for rank in range(1, number_of + 1)]
    largest = limit if full else min(limit, max(-(-total // number_of), total * portions[0] // sum(portions)))
    least = 1 if total - largest >= number_of - 1 else 0
    holding, spare = [largest] + [least] * (number_of - 1), total - largest - least * (number_of - 1)
    while spare > 0:
        free = [i for i in range(1, number_of) if holding[i] < largest] or [i for i in range(1, number_of) if holding[i] < limit]
        pool, remaining = sum([portions[i] for i in free]), spare
        for i in free:
            addition = min(limit - holding[i], max(1, remaining * portions[i] // pool), spare)
            holding[i] = holding[i] + addition
            spare = spare - addition
    return np.array(holding)


def noise(rng, extent, scale, limit, pieces=(), held_as=jnp.bfloat16):
    level = level_of(rng, extent, pieces, -0.22, 0.18) if pieces else 1.0
    values = jax.random.normal(rng, extent, jnp.float32) * scale * level
    return jnp.minimum(jnp.maximum(values, -limit), limit).astype(held_as)


def setup_inputs(seed: int = 0) -> dict:
    key_list = jax.random.split(jax.random.key(seed), 6)
    row_values = noise(key_list[0], (ROWS, F), 0.02, 0.12, ((0, 512),), jnp.float32)
    front_of_row_keys = jax.random.split(jax.random.fold_in(key_list[1], 1), ROWS // ROWS_SRC)
    front_of_row_turns = jax.random.permutation(jax.random.fold_in(key_list[1], 3), ROWS // ROWS_SRC)
    front_of_row = jax.vmap(lambda own, number: shared_out(jax.random.fold_in(key_list[1], 2), own, number, ROWS_SRC, FRONTS, 1, MOST, 2))(front_of_row_keys, front_of_row_turns).reshape((ROWS, 1))
    child_factors = draw_child_factors(jax.random.fold_in(key_list[5], 71), 0)
    child_columns = draw_child_columns(jax.random.fold_in(key_list[5], 71), 0)
    damping = jnp.clip(jnp.exp(math.log(2.0) - 1.3862944 * jax.random.uniform(key_list[4], (FRONTS, F), jnp.float32) ** level_of(key_list[4], (FRONTS, F), ((0, 128),), -0.2, 0.2)), 0.5, 2.0)
    return {"row_values": row_values, "front_of_row": front_of_row, "child_factors": child_factors, "child_columns": child_columns, "damping": damping}


HIGHEST = lax.Precision.HIGHEST

def gram_product(matrix):
    return lax.dot_general(matrix.astype(jnp.float32), matrix.astype(jnp.float32), (((0,), (0,)), ((), ())), precision=HIGHEST, preferred_element_type=jnp.float32)

def reference(row_values, front_of_row, child_factors, child_columns, damping):
    destination = front_of_row[:, 0].astype(jnp.int32)
    sorted_rows = jnp.argsort(destination, stable=True).astype(jnp.int32)
    counts = jnp.bincount(destination, length=FRONTS).astype(jnp.int32)
    starts = (jnp.cumsum(counts) - counts).astype(jnp.int32)
    capacity = MOST * N_FRONT * N_SUB
    padded_order = jnp.concatenate([sorted_rows, jnp.zeros((capacity,), jnp.int32)])
    columns = jnp.arange(F, dtype=jnp.int32)

    def factor_front(front_index):
        row_index = lax.dynamic_slice(padded_order, (starts[front_index],), (capacity,))
        is_live = jnp.arange(capacity, dtype=jnp.int32) < counts[front_index]
        front_rows = jnp.where(is_live[:, None], row_values[row_index], jnp.float32(0.0))
        gram_matrix = gram_product(front_rows)
        for child_index in range(2):
            child = child_factors[2 * front_index + child_index]
            mapping = child_columns[2 * front_index + child_index]
            spread = (mapping[:, None] == columns[None, :]).astype(jnp.float32)
            placed = jnp.dot(child.astype(jnp.float32), spread.astype(jnp.float32), precision=HIGHEST, preferred_element_type=jnp.float32)
            gram_matrix = gram_matrix + gram_product(placed)
        weight = damping[front_index]
        gram_matrix = gram_matrix + jnp.diag(weight * weight)
        return jnp.linalg.cholesky(gram_matrix).T
    return lax.map(factor_front, jnp.arange(FRONTS, dtype=jnp.int32))
```

```python
import jax
import jax.numpy as jnp
from jax import lax
from jax.experimental import pallas as pl
from jax.experimental.pallas import tpu as pltpu
from jax.sharding import PartitionSpec as P

F32 = jnp.float32
BF16 = jnp.bfloat16
BLOCK = 128
LANES = 128
GROUP = 8
MESH = pl.DeviceIdType.MESH
KEEP = (((1,), (0,)), ((), ()))
ROWS = (((0,), (0,)), ((), ()))
COLS = (((1,), (1,)), ((), ()))


def mm(left, right, dims):
    return lax.dot_general(left, right, dims, preferred_element_type=F32)


def split(x):
    high = x.astype(BF16)
    return high, (x - high.astype(F32)).astype(BF16)


def mm3(left, right, dims):
    return mm(left[0], right[0], dims) + (mm(left[0], right[1], dims) + mm(left[1], right[0], dims))


def root_of(front):
    return 2 * (front % 2) + (front // 2) % 2


def exchange_kernel(fronts, subs, rows_ref, dest_ref, child_ref, recv_ref, children_ref, slots, own_sem, send_sem, child_send, recv_sem, child_sem):
    me = lax.axis_index("front")
    sub = lax.axis_index("sub")
    rows_held = rows_ref.shape[0]
    root = root_of(me)
    chosen = (dest_ref[...] == lax.broadcasted_iota(jnp.int32, (rows_held, fronts), 1)).astype(F32)
    before = (
        lax.broadcasted_iota(jnp.int32, (rows_held, rows_held), 1)
        < lax.broadcasted_iota(jnp.int32, (rows_held, rows_held), 0)
    ).astype(BF16)
    earlier = mm(before, chosen.astype(BF16), KEEP)
    parts = split(rows_ref[...])
    per_row = rows_ref.shape[1] // LANES
    for slot in range(2):
        pick = jnp.where(earlier == slot, chosen, 0.0).astype(BF16)
        placed = mm(pick, parts[0], ROWS) + mm(pick, parts[1], ROWS)
        for k in range(per_row):
            slots[pl.ds(slot * per_row + k, fronts, stride=2 * per_row), :] = placed[:, k * LANES : (k + 1) * LANES]

    size = 2 * per_row
    mine = me * subs + sub

    def piece(front):
        return slots.at[pl.ds(pl.multiple_of(front * size, size), size), :]

    def child_copy(s):
        return pltpu.make_async_remote_copy(
            src_ref=child_ref.at[:, :, s * BLOCK :],
            dst_ref=children_ref.at[s, :, :, s * BLOCK :],
            send_sem=child_send,
            recv_sem=child_sem.at[s],
            device_id=(me, root),
            device_id_type=MESH,
        )

    for s in range(subs):

        @pl.when((sub == s) & (root != s))
        def _():
            child_copy(s).start()

    def send(i, carry):
        front = lax.rem(me + i, fronts)
        target = root_of(front)

        @pl.when((front != me) | (target != sub))
        def _():
            pltpu.make_async_remote_copy(
                src_ref=piece(front),
                dst_ref=recv_ref.at[mine],
                send_sem=send_sem,
                recv_sem=recv_sem,
                device_id=(front, target),
                device_id_type=MESH,
            ).start()

        return carry

    lax.fori_loop(0, fronts, send, 0)
    for s in range(subs):

        @pl.when((sub == s) & (root == s))
        def _():
            own = pltpu.make_async_copy(piece(me), recv_ref.at[mine], own_sem.at[0])
            own.start()
            kids = pltpu.make_async_copy(
                child_ref.at[:, :, s * BLOCK :], children_ref.at[s, :, :, s * BLOCK :], own_sem.at[1]
            )
            kids.start()
            own.wait()
            kids.wait()
            everyone = recv_ref.at[pl.ds(0, fronts * subs - 1)]
            pltpu.make_async_copy(everyone, everyone, recv_sem).wait()
            for other in range(subs):
                if other != s:
                    child_copy(other).wait_recv()
            sent = slots.at[pl.ds(0, (fronts - 1) * size), :]
            pltpu.make_async_copy(sent, sent, send_sem).wait()

        @pl.when((sub == s) & (root != s))
        def _():
            child_copy(s).wait_send()
            pltpu.make_async_copy(slots, slots, send_sem).wait()


def exchange(rows, dest, child, fronts, subs):
    rows_held, width = rows.shape
    per_row = width // LANES
    size = 2 * per_row
    return pl.pallas_call(
        lambda *refs: exchange_kernel(fronts, subs, *refs),
        out_shape=[
            jax.ShapeDtypeStruct((fronts * subs, size, LANES), F32),
            jax.ShapeDtypeStruct((subs,) + child.shape, F32),
        ],
        in_specs=[
            pl.BlockSpec(memory_space=pltpu.VMEM),
            pl.BlockSpec(memory_space=pltpu.VMEM),
            pl.BlockSpec(memory_space=pl.ANY),
        ],
        out_specs=[pl.BlockSpec(memory_space=pl.ANY)] * 2,
        scratch_shapes=[
            pltpu.VMEM((fronts * size, LANES), F32),
            pltpu.SemaphoreType.DMA((2,)),
            pltpu.SemaphoreType.DMA,
            pltpu.SemaphoreType.DMA,
            pltpu.SemaphoreType.DMA,
            pltpu.SemaphoreType.DMA((subs,)),
        ],
        compiler_params=pltpu.CompilerParams(has_side_effects=True),
        name="ray_exchange",
    )(rows, dest, child)


def lane_copy(x, j):
    return jnp.broadcast_to(x[:, j : j + 1], (GROUP, LANES))


def row_copy(x, j):
    return jnp.broadcast_to(x[j : j + 1, :], (GROUP, LANES))


def factor_block(source, upper_ref, inverse_ref):
    count = BLOCK // GROUP
    sub = lax.broadcasted_iota(jnp.int32, (GROUP, LANES), 0)
    lane = lax.broadcasted_iota(jnp.int32, (GROUP, LANES), 1)
    a = [source[GROUP * k : GROUP * (k + 1), :] for k in range(count)]
    e = [jnp.where(lane == sub + GROUP * k, 1.0, 0.0).astype(F32) for k in range(count)]
    for k in range(count):
        b = [lane_copy(a[k], GROUP * k + m) for m in range(GROUP)]
        pivots = None
        u = [[None] * GROUP for _ in range(GROUP)]
        inv = [None] * GROUP
        for j in range(GROUP):
            pivot = row_copy(b[j], j)
            pivots = pivot if pivots is None else jnp.where(sub >= j, pivot, pivots)
            inv[j] = 1.0 / pivot
            ratio = jnp.where(sub > j, b[j], 0.0) * inv[j]
            for m in range(j + 1, GROUP):
                u[j][m] = row_copy(b[m], j)
                b[m] = b[m] - ratio * u[j][m]
            a[k] = a[k] - ratio * row_copy(a[k], j)
            e[k] = e[k] - ratio * row_copy(e[k], j)
        scale = lax.rsqrt(pivots)
        upper_ref[GROUP * k : GROUP * (k + 1), :] = a[k] * scale
        inverse_ref[GROUP * k : GROUP * (k + 1), :] = e[k] * scale
        rows_a = [row_copy(a[k], j) for j in range(GROUP)]
        rows_e = [row_copy(e[k], j) for j in range(GROUP)]
        for q in range(k + 1, count):
            c = [lane_copy(a[q], GROUP * k + m) for m in range(GROUP)]
            for j in range(GROUP):
                ratio = c[j] * inv[j]
                for m in range(j + 1, GROUP):
                    c[m] = c[m] - ratio * u[j][m]
                a[q] = a[q] - ratio * rows_a[j]
                e[q] = e[q] - ratio * rows_e[j]


def factor_kernel(recv_ref, children_ref, columns_ref, damping_ref, r_ref, xh, xl, rh, rl, panel, block, upper, inverse):
    width = r_ref.shape[1]
    per_row = width // LANES
    rays = recv_ref.shape[0] // per_row
    subs, kids, _, contrib = children_ref.shape
    me = lax.axis_index("front")
    sub = lax.axis_index("sub")

    @pl.when(sub == root_of(me))
    def _():
        def take(i, carry):
            base = pl.multiple_of(i * BLOCK, BLOCK)
            for k in range(per_row):
                high, low = split(recv_ref[pl.ds(base * per_row + k, BLOCK, stride=per_row), :])
                xh[pl.ds(base, BLOCK), k * LANES : (k + 1) * LANES] = high
                xl[pl.ds(base, BLOCK), k * LANES : (k + 1) * LANES] = low
            return carry

        lax.fori_loop(0, rays // BLOCK, take, 0)
        for c in range(kids):
            spread = (
                lax.broadcasted_iota(jnp.int32, (width, contrib), 0) == columns_ref[c : c + 1, :]
            ).astype(F32).astype(BF16)
            for s in range(subs):
                high, low = split(children_ref[s, c, :, s * BLOCK :])
                at = rays + c * contrib + s * BLOCK
                xh[at : at + BLOCK, :] = mm(high, spread[:, s * BLOCK :], COLS).astype(BF16)
                xl[at : at + BLOCK, :] = mm(low, spread[:, s * BLOCK :], COLS).astype(BF16)
        on_diagonal = lax.broadcasted_iota(jnp.int32, (BLOCK, BLOCK), 0) == lax.broadcasted_iota(
            jnp.int32, (BLOCK, BLOCK), 1
        )

        def step(i, carry):
            for b in range(width // BLOCK):

                @pl.when(i == b)
                def _():
                    c0, c1 = b * BLOCK, (b + 1) * BLOCK
                    acc = mm3((xh[:, c0:c1], xl[:, c0:c1]), (xh[:, c0:], xl[:, c0:]), ROWS)
                    if b:
                        acc = acc - mm3((rh[:c0, c0:c1], rl[:c0, c0:c1]), (rh[:c0, c0:], rl[:c0, c0:]), ROWS)
                    panel[:, c0:] = acc
                    weight = damping_ref[:, c0:c1]
                    block[...] = acc[:, :BLOCK] + jnp.where(on_diagonal, weight * weight, 0.0)

            factor_block(block, upper, inverse)
            for b in range(width // BLOCK):

                @pl.when(i == b)
                def _():
                    c0, c1 = b * BLOCK, (b + 1) * BLOCK
                    if b:
                        r_ref[c0:c1, :c0] = jnp.zeros((BLOCK, c0), F32)
                    r_ref[c0:c1, c0:c1] = upper[...]
                    if c1 < width:
                        rest = mm3(split(inverse[...]), split(panel[:, c1:]), KEEP)
                        r_ref[c0:c1, c1:] = rest
                        rh[c0:c1, c1:], rl[c0:c1, c1:] = split(rest)

            return carry

        lax.fori_loop(0, width // BLOCK, step, 0)


def factor(recv, children, columns, damping):
    width = damping.shape[1]
    total = recv.shape[0] * LANES // width + children.shape[1] * children.shape[3]
    return pl.pallas_call(
        factor_kernel,
        out_shape=jax.ShapeDtypeStruct((width, width), F32),
        in_specs=[pl.BlockSpec(memory_space=pltpu.VMEM)] * 4,
        out_specs=pl.BlockSpec(memory_space=pltpu.VMEM),
        scratch_shapes=[
            pltpu.VMEM((total, width), BF16),
            pltpu.VMEM((total, width), BF16),
            pltpu.VMEM((width, width), BF16),
            pltpu.VMEM((width, width), BF16),
            pltpu.VMEM((BLOCK, width), F32),
            pltpu.VMEM((BLOCK, BLOCK), F32),
            pltpu.VMEM((BLOCK, BLOCK), F32),
            pltpu.VMEM((BLOCK, BLOCK), F32),
        ],
        name="front_factor",
    )(recv, children, columns, damping)


def spread_kernel(subs, r_ref, out_ref, send_sem, recv_sem, own_sem):
    me = lax.axis_index("front")
    sub = lax.axis_index("sub")
    root = root_of(me)
    rows = out_ref.shape[0]
    barrier = pltpu.get_barrier_semaphore()

    @pl.when(sub != root)
    def _():
        pl.semaphore_signal(barrier, inc=1, device_id=(me, root), device_id_type=MESH)

    @pl.when(sub == root)
    def _():
        pl.semaphore_wait(barrier, subs - 1)

    def copy(s):
        return pltpu.make_async_remote_copy(
            src_ref=r_ref.at[s * rows : (s + 1) * rows, :],
            dst_ref=out_ref,
            send_sem=send_sem.at[s],
            recv_sem=recv_sem,
            device_id=(me, s),
            device_id_type=MESH,
        )

    for r in range(subs):

        @pl.when((sub == r) & (root == r))
        def _():
            for s in range(subs):
                if s != r:
                    copy(s).start()
            own = pltpu.make_async_copy(r_ref.at[r * rows : (r + 1) * rows, :], out_ref, own_sem)
            own.start()
            own.wait()
            for s in range(subs):
                if s != r:
                    copy(s).wait_send()

        @pl.when((sub == r) & (root != r))
        def _():
            copy(r).wait_recv()


def spread_rows(r, subs):
    width = r.shape[0]
    return pl.pallas_call(
        lambda *refs: spread_kernel(subs, *refs),
        out_shape=jax.ShapeDtypeStruct((width // subs, width), F32),
        in_specs=[pl.BlockSpec(memory_space=pl.ANY)],
        out_specs=pl.BlockSpec(memory_space=pl.ANY),
        scratch_shapes=[
            pltpu.SemaphoreType.DMA((subs,)),
            pltpu.SemaphoreType.DMA,
            pltpu.SemaphoreType.DMA,
        ],
        compiler_params=pltpu.CompilerParams(collective_id=1, has_side_effects=True),
        name="factor_rows_out",
    )(r)


def local(row_values, front_of_row, child_factors, child_columns, damping):
    fronts = lax.axis_size("front")
    subs = lax.axis_size("sub")
    recv, children = exchange(row_values, front_of_row, child_factors, fronts, subs)
    recv = recv.reshape((-1, LANES))
    r = factor(recv, children, child_columns, damping)
    return spread_rows(r, subs)[None]


def solution(mesh):
    in_specs = (
        P(("front", "sub"), None),
        P(("front", "sub"), None),
        P("front", "sub", None),
        P("front", None),
        P("front", None),
    )
    out_specs = P("front", "sub", None)
    return jax.shard_map(local, mesh=mesh, in_specs=in_specs, out_specs=out_specs, check_vma=False)
```

```python
import jax
import jax.numpy as jnp
from jax import lax
from jax.experimental import pallas as pl
from jax.experimental.pallas import tpu as pltpu
from jax.sharding import PartitionSpec as P

F32 = jnp.float32
BF16 = jnp.bfloat16
BLOCK = 128
LANES = 128
GROUP = 8
GROUPS = 4
STRIDE = 53
MESH = pl.DeviceIdType.MESH
KEEP = (((1,), (0,)), ((), ()))
ROWS = (((0,), (0,)), ((), ()))
COLS = (((1,), (1,)), ((), ()))


def mm(left, right, dims):
    return lax.dot_general(left, right, dims, preferred_element_type=F32)


def split(x):
    high = x.astype(BF16)
    return high, (x - high.astype(F32)).astype(BF16)


def mm3(left, right, dims):
    return mm(left[0], right[0], dims) + (mm(left[0], right[1], dims) + mm(left[1], right[0], dims))


def root_of(front):
    return lax.rem(2 * (front % 2) + (front // 2) % 2 + front // 4 + front // 16, 4)


def lane_copy(x, j):
    return jnp.broadcast_to(x[:, j : j + 1], (GROUP, LANES))


def row_copy(x, j):
    return jnp.broadcast_to(x[j : j + 1, :], (GROUP, LANES))


def factor_block(source, upper_ref, inverse_ref):
    count = BLOCK // GROUP
    sub = lax.broadcasted_iota(jnp.int32, (GROUP, LANES), 0)
    lane = lax.broadcasted_iota(jnp.int32, (GROUP, LANES), 1)
    a = [source[GROUP * k : GROUP * (k + 1), :] for k in range(count)]
    e = [jnp.where(lane == sub + GROUP * k, 1.0, 0.0).astype(F32) for k in range(count)]
    for k in range(count):
        b = [lane_copy(a[k], GROUP * k + m) for m in range(GROUP)]
        pivots = None
        u = [[None] * GROUP for _ in range(GROUP)]
        inv = [None] * GROUP
        for j in range(GROUP):
            pivot = row_copy(b[j], j)
            pivots = pivot if pivots is None else jnp.where(sub >= j, pivot, pivots)
            inv[j] = 1.0 / pivot
            ratio = jnp.where(sub > j, b[j], 0.0) * inv[j]
            for m in range(j + 1, GROUP):
                u[j][m] = row_copy(b[m], j)
                b[m] = b[m] - ratio * u[j][m]
            a[k] = a[k] - ratio * row_copy(a[k], j)
            e[k] = e[k] - ratio * row_copy(e[k], j)
        scale = lax.rsqrt(pivots)
        upper_ref[GROUP * k : GROUP * (k + 1), :] = a[k] * scale
        inverse_ref[GROUP * k : GROUP * (k + 1), :] = e[k] * scale
        rows_a = [row_copy(a[k], j) for j in range(GROUP)]
        rows_e = [row_copy(e[k], j) for j in range(GROUP)]
        for q in range(k + 1, count):
            c = [lane_copy(a[q], GROUP * k + m) for m in range(GROUP)]
            for j in range(GROUP):
                ratio = c[j] * inv[j]
                for m in range(j + 1, GROUP):
                    c[m] = c[m] - ratio * u[j][m]
                a[q] = a[q] - ratio * rows_a[j]
                e[q] = e[q] - ratio * rows_e[j]


def merge_kernel(
    fronts,
    subs,
    rows_ref,
    dest_ref,
    child_ref,
    columns_ref,
    damping_ref,
    out_ref,
    slots,
    recv,
    children,
    zeros,
    xh,
    xl,
    gram,
    r_full,
    rh,
    rl,
    block,
    upper,
    inverse,
    send_sem,
    recv_sem,
    child_send,
    child_recv,
    child_own,
    fill_sem,
    row_send,
    row_recv,
):
    me = lax.axis_index("front")
    sub = lax.axis_index("sub")
    root = root_of(me)
    rows_held, width = rows_ref.shape
    kids, _, contrib = child_ref.shape
    per_row = width // LANES
    size = 2 * per_row
    groups = recv_sem.shape[0]
    blocks = width // BLOCK
    per_sub = blocks // subs

    def child_copy(s):
        return pltpu.make_async_remote_copy(
            src_ref=child_ref.at[:, :, s * BLOCK :],
            dst_ref=children.at[s, :, :, s * BLOCK :],
            send_sem=child_send,
            recv_sem=child_recv.at[s],
            device_id=(me, root),
            device_id_type=MESH,
        )

    def child_keep(s):
        return pltpu.make_async_copy(child_ref.at[:, :, s * BLOCK :], children.at[s, :, :, s * BLOCK :], child_own)

    for s in range(subs):

        @pl.when((sub == s) & (root != s))
        def _():
            child_copy(s).start()

        @pl.when((sub == s) & (root == s))
        def _():
            child_keep(s).start()

    def fill(b):
        half = b % per_sub
        return pltpu.make_async_copy(
            zeros.at[:, : b * BLOCK], out_ref.at[half * BLOCK : (half + 1) * BLOCK, : b * BLOCK], fill_sem.at[half]
        )

    zeros[...] = jnp.zeros_like(zeros)

    chosen = (dest_ref[...] == lax.broadcasted_iota(jnp.int32, (rows_held, fronts), 1)).astype(F32)
    before = (
        lax.broadcasted_iota(jnp.int32, (rows_held, rows_held), 1)
        < lax.broadcasted_iota(jnp.int32, (rows_held, rows_held), 0)
    ).astype(BF16)
    earlier = mm(before, chosen.astype(BF16), KEEP)
    parts = split(rows_ref[...])
    for slot in range(2):
        pick = jnp.where(earlier == slot, chosen, 0.0).astype(BF16)
        placed = mm(pick, parts[0], ROWS) + mm(pick, parts[1], ROWS)
        for k in range(per_row):
            slots[pl.ds(slot * per_row + k, fronts, stride=size), :] = placed[:, k * LANES : (k + 1) * LANES]

    def piece(front):
        return slots.at[pl.ds(pl.multiple_of(front * size, size), size), :]

    steps = fronts // groups
    for g in range(groups):

        def send(i, carry):
            front = lax.rem(me + STRIDE * i, fronts)
            target = root_of(front)

            @pl.when((front != me) | (target != sub))
            def _():
                pltpu.make_async_remote_copy(
                    src_ref=piece(front),
                    dst_ref=recv.at[pl.ds(pl.multiple_of((i * subs + sub) * size, size), size), :],
                    send_sem=send_sem,
                    recv_sem=recv_sem.at[g],
                    device_id=(front, target),
                    device_id_type=MESH,
                ).start()

            return carry

        lax.fori_loop(g * steps, (g + 1) * steps, send, 0)

    for b in range(blocks):
        if b:

            @pl.when(sub == b // per_sub)
            def _():
                fill(b).start()

    def row_copy_out(b):
        half = b % per_sub
        return pltpu.make_async_remote_copy(
            src_ref=r_full.at[b * BLOCK : (b + 1) * BLOCK, b * BLOCK :],
            dst_ref=out_ref.at[half * BLOCK : (half + 1) * BLOCK, b * BLOCK :],
            send_sem=row_send.at[b],
            recv_sem=row_recv.at[half],
            device_id=(me, b // per_sub),
            device_id_type=MESH,
        )

    def row_keep(b):
        half = b % per_sub
        return pltpu.make_async_copy(
            r_full.at[b * BLOCK : (b + 1) * BLOCK, b * BLOCK :],
            out_ref.at[half * BLOCK : (half + 1) * BLOCK, b * BLOCK :],
            row_send.at[b],
        )

    @pl.when(sub == root)
    def _():
        recv[pl.ds(pl.multiple_of(sub * size, size), size), :] = slots[pl.ds(pl.multiple_of(me * size, size), size), :]
        for s in range(subs):

            @pl.when(root == s)
            def _():
                child_keep(s).wait()

            @pl.when(root != s)
            def _():
                child_copy(s).wait_recv()

        for c in range(kids):
            spread = (
                lax.broadcasted_iota(jnp.int32, (width, contrib), 0) == columns_ref[c : c + 1, :]
            ).astype(F32).astype(BF16)
            for s in range(subs):
                high, low = split(children[s, c, :, s * BLOCK :])
                at = c * contrib + s * BLOCK
                xh[at : at + BLOCK, :] = mm(high, spread[:, s * BLOCK :], COLS).astype(BF16)
                xl[at : at + BLOCK, :] = mm(low, spread[:, s * BLOCK :], COLS).astype(BF16)
        on_diagonal = lax.broadcasted_iota(jnp.int32, (BLOCK, BLOCK), 0) == lax.broadcasted_iota(
            jnp.int32, (BLOCK, BLOCK), 1
        )
        for b in range(blocks):
            c0, c1 = b * BLOCK, (b + 1) * BLOCK
            gram[c0:c1, c0:] = mm3((xh[:, c0:c1], xl[:, c0:c1]), (xh[:, c0:], xl[:, c0:]), ROWS)
            weight = damping_ref[:, c0:c1]
            gram[c0:c1, c0:c1] += jnp.where(on_diagonal, weight * weight, 0.0)

        slots_in = steps * subs
        count = 2 * slots_in

        def gather(g, carry):
            for h in range(groups):

                @pl.when(g == h)
                def _():
                    first = 1 if h == 0 else 0
                    region = recv.at[pl.ds(0, (slots_in - first) * size), :]
                    pltpu.make_async_copy(region, region, recv_sem.at[h]).wait()

            for q in range(count // BLOCK):
                base = pl.multiple_of(g * count + q * BLOCK, BLOCK)
                for k in range(per_row):
                    high, low = split(recv[pl.ds(base * per_row + k, BLOCK, stride=per_row), :])
                    xh[q * BLOCK : (q + 1) * BLOCK, k * LANES : (k + 1) * LANES] = high
                    xl[q * BLOCK : (q + 1) * BLOCK, k * LANES : (k + 1) * LANES] = low
            for b in range(blocks):
                c0, c1 = b * BLOCK, (b + 1) * BLOCK
                gram[c0:c1, c0:] += mm3(
                    (xh[:count, c0:c1], xl[:count, c0:c1]), (xh[:count, c0:], xl[:count, c0:]), ROWS
                )
            return carry

        lax.fori_loop(0, groups, gather, 0)

        def step(i, carry):
            for b in range(blocks):

                @pl.when(i == b)
                def _():
                    c0, c1 = b * BLOCK, (b + 1) * BLOCK
                    if b:
                        gram[c0:c1, c0:] -= mm3(
                            (rh[:c0, c0:c1], rl[:c0, c0:c1]), (rh[:c0, c0:], rl[:c0, c0:]), ROWS
                        )
                    block[...] = gram[c0:c1, c0:c1]

            factor_block(block, upper, inverse)
            for b in range(blocks):

                @pl.when(i == b)
                def _():
                    c0, c1 = b * BLOCK, (b + 1) * BLOCK
                    r_full[c0:c1, c0:c1] = upper[...]
                    if c1 < width:
                        rest = mm3(split(inverse[...]), split(gram[c0:c1, c1:]), KEEP)
                        r_full[c0:c1, c1:] = rest
                        rh[c0:c1, c1:], rl[c0:c1, c1:] = split(rest)

                    @pl.when(root != b // per_sub)
                    def _():
                        row_copy_out(b).start()

                    @pl.when(root == b // per_sub)
                    def _():
                        row_keep(b).start()

            return carry

        lax.fori_loop(0, blocks, step, 0)
        for b in range(blocks):

            @pl.when(root != b // per_sub)
            def _():
                row_copy_out(b).wait_send()

            @pl.when(root == b // per_sub)
            def _():
                row_keep(b).wait()

        sent = slots.at[pl.ds(0, (fronts - 1) * size), :]
        pltpu.make_async_copy(sent, sent, send_sem).wait()

    @pl.when(sub != root)
    def _():
        for s in range(subs):

            @pl.when(sub == s)
            def _():
                child_copy(s).wait_send()
                for b in range(s * per_sub, (s + 1) * per_sub):
                    row_copy_out(b).wait_recv()

        pltpu.make_async_copy(slots, slots, send_sem).wait()

    for b in range(blocks):
        if b:

            @pl.when(sub == b // per_sub)
            def _():
                fill(b).wait()


def merge(rows, dest, child, columns, damping, fronts, subs):
    rows_held, width = rows.shape
    size = 2 * width // LANES
    kids, _, contrib = child.shape
    groups = GROUPS
    deep = max(kids * contrib, 2 * fronts * subs // groups)
    blocks = width // BLOCK
    vmem = pl.BlockSpec(memory_space=pltpu.VMEM)
    return pl.pallas_call(
        lambda *refs: merge_kernel(fronts, subs, *refs),
        out_shape=jax.ShapeDtypeStruct((width // subs, width), F32),
        in_specs=[vmem, vmem, pl.BlockSpec(memory_space=pl.ANY), vmem, vmem],
        out_specs=pl.BlockSpec(memory_space=pl.ANY),
        scratch_shapes=[
            pltpu.VMEM((fronts * size, LANES), F32),
            pltpu.VMEM((fronts * subs * size, LANES), F32),
            pltpu.VMEM((subs,) + child.shape, F32),
            pltpu.VMEM((BLOCK, width), F32),
            pltpu.VMEM((deep, width), BF16),
            pltpu.VMEM((deep, width), BF16),
            pltpu.VMEM((width, width), F32),
            pltpu.VMEM((width, width), F32),
            pltpu.VMEM((width, width), BF16),
            pltpu.VMEM((width, width), BF16),
            pltpu.VMEM((BLOCK, BLOCK), F32),
            pltpu.VMEM((BLOCK, BLOCK), F32),
            pltpu.VMEM((BLOCK, BLOCK), F32),
            pltpu.SemaphoreType.DMA,
            pltpu.SemaphoreType.DMA((groups,)),
            pltpu.SemaphoreType.DMA,
            pltpu.SemaphoreType.DMA((subs,)),
            pltpu.SemaphoreType.DMA,
            pltpu.SemaphoreType.DMA((blocks // subs,)),
            pltpu.SemaphoreType.DMA((blocks,)),
            pltpu.SemaphoreType.DMA((blocks // subs,)),
        ],
        compiler_params=pltpu.CompilerParams(has_side_effects=True),
        name="front_merge",
    )(rows, dest, child, columns, damping)


def local(row_values, front_of_row, child_factors, child_columns, damping):
    fronts = lax.axis_size("front")
    subs = lax.axis_size("sub")
    return merge(row_values, front_of_row, child_factors, child_columns, damping, fronts, subs)[None]


def solution(mesh):
    in_specs = (
        P(("front", "sub"), None),
        P(("front", "sub"), None),
        P("front", "sub", None),
        P("front", None),
        P("front", None),
    )
    out_specs = P("front", "sub", None)
    return jax.shard_map(local, mesh=mesh, in_specs=in_specs, out_specs=out_specs, check_vma=False)
```

```python
import jax
import jax.numpy as jnp
from jax import lax
from jax.experimental import pallas as pl
from jax.experimental.pallas import tpu as pltpu
from jax.sharding import PartitionSpec as P

F32 = jnp.float32
BF16 = jnp.bfloat16
BLOCK = 128
LANES = 128
GROUP = 8
GROUPS = 4
STRIDE = 53
MESH = pl.DeviceIdType.MESH
KEEP = (((1,), (0,)), ((), ()))
ROWS = (((0,), (0,)), ((), ()))
COLS = (((1,), (1,)), ((), ()))


def mm(left, right, dims):
    return lax.dot_general(left, right, dims, preferred_element_type=F32)


def split(x):
    high = x.astype(BF16)
    return high, (x - high.astype(F32)).astype(BF16)


def mm3(left, right, dims):
    return mm(left[0], right[0], dims) + (mm(left[0], right[1], dims) + mm(left[1], right[0], dims))


def root_of(front):
    return lax.rem(2 * (front % 2) + (front // 2) % 2 + front // 4 + front // 16, 4)


def lane_copy(x, j):
    return jnp.broadcast_to(x[:, j : j + 1], (GROUP, LANES))


def row_copy(x, j):
    return jnp.broadcast_to(x[j : j + 1, :], (GROUP, LANES))


def factor_block(source, upper_ref, inverse_ref):
    count = BLOCK // GROUP
    sub = lax.broadcasted_iota(jnp.int32, (GROUP, LANES), 0)
    lane = lax.broadcasted_iota(jnp.int32, (GROUP, LANES), 1)
    a = [source[GROUP * k : GROUP * (k + 1), :] for k in range(count)]
    e = [jnp.where(lane == sub + GROUP * k, 1.0, 0.0).astype(F32) for k in range(count)]
    for k in range(count):
        b = [lane_copy(a[k], GROUP * k + m) for m in range(GROUP)]
        pivots = None
        u = [[None] * GROUP for _ in range(GROUP)]
        inv = [None] * GROUP
        for j in range(GROUP):
            pivot = row_copy(b[j], j)
            pivots = pivot if pivots is None else jnp.where(sub >= j, pivot, pivots)
            inv[j] = 1.0 / pivot
            ratio = jnp.where(sub > j, b[j], 0.0) * inv[j]
            for m in range(j + 1, GROUP):
                u[j][m] = row_copy(b[m], j)
                b[m] = b[m] - ratio * u[j][m]
            a[k] = a[k] - ratio * row_copy(a[k], j)
            e[k] = e[k] - ratio * row_copy(e[k], j)
        scale = lax.rsqrt(pivots)
        upper_ref[GROUP * k : GROUP * (k + 1), :] = a[k] * scale
        inverse_ref[GROUP * k : GROUP * (k + 1), :] = e[k] * scale
        rows_a = [row_copy(a[k], j) for j in range(GROUP)]
        rows_e = [row_copy(e[k], j) for j in range(GROUP)]
        for q in range(k + 1, count):
            c = [lane_copy(a[q], GROUP * k + m) for m in range(GROUP)]
            for j in range(GROUP):
                ratio = c[j] * inv[j]
                for m in range(j + 1, GROUP):
                    c[m] = c[m] - ratio * u[j][m]
                a[q] = a[q] - ratio * rows_a[j]
                e[q] = e[q] - ratio * rows_e[j]


def merge_kernel(
    fronts,
    subs,
    rows_ref,
    dest_ref,
    child_ref,
    columns_ref,
    damping_ref,
    out_ref,
    slots,
    away,
    pairs,
    recv,
    children,
    zeros,
    xh,
    xl,
    gram,
    r_full,
    rh,
    rl,
    block,
    upper,
    inverse,
    pair_send,
    pair_recv,
    send_sem,
    recv_sem,
    child_send,
    child_recv,
    child_own,
    fill_sem,
    row_send,
    row_recv,
):
    me = lax.axis_index("front")
    sub = lax.axis_index("sub")
    root = root_of(me)
    rows_held, width = rows_ref.shape
    kids, _, contrib = child_ref.shape
    per_row = width // LANES
    size = 2 * per_row
    groups = recv_sem.shape[0]
    blocks = width // BLOCK
    per_sub = blocks // subs

    def child_copy(s):
        return pltpu.make_async_remote_copy(
            src_ref=child_ref.at[:, :, s * BLOCK :],
            dst_ref=children.at[s, :, :, s * BLOCK :],
            send_sem=child_send,
            recv_sem=child_recv.at[s],
            device_id=(me, root),
            device_id_type=MESH,
        )

    def child_keep(s):
        return pltpu.make_async_copy(child_ref.at[:, :, s * BLOCK :], children.at[s, :, :, s * BLOCK :], child_own)

    for s in range(subs):

        @pl.when((sub == s) & (root != s))
        def _():
            child_copy(s).start()

        @pl.when((sub == s) & (root == s))
        def _():
            child_keep(s).start()

    def fill(b):
        half = b % per_sub
        return pltpu.make_async_copy(
            zeros.at[:, : b * BLOCK], out_ref.at[half * BLOCK : (half + 1) * BLOCK, : b * BLOCK], fill_sem.at[half]
        )

    zeros[...] = jnp.zeros_like(zeros)

    core = lax.rem(me, 2)
    pair = me // 2
    half = fronts // 2
    place = lax.broadcasted_iota(jnp.int32, (rows_held, fronts), 1)
    late = place >= half
    name = jnp.where(late, 2 * (place - half) + (1 - core), 2 * place + core)
    chosen = (dest_ref[...] == name).astype(F32)
    before = (
        lax.broadcasted_iota(jnp.int32, (rows_held, rows_held), 1)
        < lax.broadcasted_iota(jnp.int32, (rows_held, rows_held), 0)
    ).astype(BF16)
    earlier = mm(before, chosen.astype(BF16), KEEP)
    parts = split(rows_ref[...])
    for slot in range(2):
        pick = jnp.where(earlier == slot, chosen, 0.0).astype(BF16)
        placed = mm(pick, parts[0], ROWS) + mm(pick, parts[1], ROWS)
        for k in range(per_row):
            slots[pl.ds(slot * per_row + k, fronts, stride=size), :] = placed[:, k * LANES : (k + 1) * LANES]
    for j in range(half):
        pairs[j, :size, :] = slots[j * size : (j + 1) * size, :]
        away[j] = slots[(half + j) * size : (half + j + 1) * size, :]

    swap = pltpu.make_async_remote_copy(
        src_ref=away,
        dst_ref=pairs.at[:, size:, :],
        send_sem=pair_send,
        recv_sem=pair_recv,
        device_id=(me + 1 - 2 * core, sub),
        device_id_type=MESH,
    )
    swap.start()
    swap.wait()
    steps = half // groups
    for g in range(groups):

        def send(i, carry):
            to = lax.rem(pair + STRIDE * i, half)
            front = 2 * to + core
            target = root_of(front)

            @pl.when((front != me) | (target != sub))
            def _():
                pltpu.make_async_remote_copy(
                    src_ref=pairs.at[to],
                    dst_ref=recv.at[pl.ds(pl.multiple_of((i * subs + sub) * 2 * size, 2 * size), 2 * size), :],
                    send_sem=send_sem,
                    recv_sem=recv_sem.at[g],
                    device_id=(front, target),
                    device_id_type=MESH,
                ).start()

            return carry

        lax.fori_loop(g * steps, (g + 1) * steps, send, 0)

    for b in range(blocks):
        if b:

            @pl.when(sub == b // per_sub)
            def _():
                fill(b).start()

    def row_copy_out(b):
        half = b % per_sub
        return pltpu.make_async_remote_copy(
            src_ref=r_full.at[b * BLOCK : (b + 1) * BLOCK, b * BLOCK :],
            dst_ref=out_ref.at[half * BLOCK : (half + 1) * BLOCK, b * BLOCK :],
            send_sem=row_send.at[b],
            recv_sem=row_recv.at[half],
            device_id=(me, b // per_sub),
            device_id_type=MESH,
        )

    def row_keep(b):
        half = b % per_sub
        return pltpu.make_async_copy(
            r_full.at[b * BLOCK : (b + 1) * BLOCK, b * BLOCK :],
            out_ref.at[half * BLOCK : (half + 1) * BLOCK, b * BLOCK :],
            row_send.at[b],
        )

    @pl.when(sub == root)
    def _():
        recv[pl.ds(pl.multiple_of(sub * 2 * size, 2 * size), 2 * size), :] = pairs[pair]
        for s in range(subs):

            @pl.when(root == s)
            def _():
                child_keep(s).wait()

            @pl.when(root != s)
            def _():
                child_copy(s).wait_recv()

        for c in range(kids):
            spread = (
                lax.broadcasted_iota(jnp.int32, (width, contrib), 0) == columns_ref[c : c + 1, :]
            ).astype(F32).astype(BF16)
            for s in range(subs):
                high, low = split(children[s, c, :, s * BLOCK :])
                at = c * contrib + s * BLOCK
                xh[at : at + BLOCK, :] = mm(high, spread[:, s * BLOCK :], COLS).astype(BF16)
                xl[at : at + BLOCK, :] = mm(low, spread[:, s * BLOCK :], COLS).astype(BF16)
        on_diagonal = lax.broadcasted_iota(jnp.int32, (BLOCK, BLOCK), 0) == lax.broadcasted_iota(
            jnp.int32, (BLOCK, BLOCK), 1
        )
        for b in range(blocks):
            c0, c1 = b * BLOCK, (b + 1) * BLOCK
            gram[c0:c1, c0:] = mm3((xh[:, c0:c1], xl[:, c0:c1]), (xh[:, c0:], xl[:, c0:]), ROWS)
            weight = damping_ref[:, c0:c1]
            gram[c0:c1, c0:c1] += jnp.where(on_diagonal, weight * weight, 0.0)

        slots_in = steps * subs
        count = 4 * slots_in

        def gather(g, carry):
            for h in range(groups):

                @pl.when(g == h)
                def _():
                    first = 1 if h == 0 else 0
                    region = recv.at[pl.ds(0, (slots_in - first) * 2 * size), :]
                    pltpu.make_async_copy(region, region, recv_sem.at[h]).wait()

            for q in range(count // BLOCK):
                base = pl.multiple_of(g * count + q * BLOCK, BLOCK)
                for k in range(per_row):
                    high, low = split(recv[pl.ds(base * per_row + k, BLOCK, stride=per_row), :])
                    xh[q * BLOCK : (q + 1) * BLOCK, k * LANES : (k + 1) * LANES] = high
                    xl[q * BLOCK : (q + 1) * BLOCK, k * LANES : (k + 1) * LANES] = low
            for b in range(blocks):
                c0, c1 = b * BLOCK, (b + 1) * BLOCK
                gram[c0:c1, c0:] += mm3(
                    (xh[:count, c0:c1], xl[:count, c0:c1]), (xh[:count, c0:], xl[:count, c0:]), ROWS
                )
            return carry

        lax.fori_loop(0, groups, gather, 0)

        def step(i, carry):
            for b in range(blocks):

                @pl.when(i == b)
                def _():
                    c0, c1 = b * BLOCK, (b + 1) * BLOCK
                    if b:
                        gram[c0:c1, c0:] -= mm3(
                            (rh[:c0, c0:c1], rl[:c0, c0:c1]), (rh[:c0, c0:], rl[:c0, c0:]), ROWS
                        )
                    block[...] = gram[c0:c1, c0:c1]

            factor_block(block, upper, inverse)
            for b in range(blocks):

                @pl.when(i == b)
                def _():
                    c0, c1 = b * BLOCK, (b + 1) * BLOCK
                    r_full[c0:c1, c0:c1] = upper[...]
                    if c1 < width:
                        rest = mm3(split(inverse[...]), split(gram[c0:c1, c1:]), KEEP)
                        r_full[c0:c1, c1:] = rest
                        rh[c0:c1, c1:], rl[c0:c1, c1:] = split(rest)

                    @pl.when(root != b // per_sub)
                    def _():
                        row_copy_out(b).start()

                    @pl.when(root == b // per_sub)
                    def _():
                        row_keep(b).start()

            return carry

        lax.fori_loop(0, blocks, step, 0)
        for b in range(blocks):

            @pl.when(root != b // per_sub)
            def _():
                row_copy_out(b).wait_send()

            @pl.when(root == b // per_sub)
            def _():
                row_keep(b).wait()

        sent = pairs.at[pl.ds(0, half - 1)]
        pltpu.make_async_copy(sent, sent, send_sem).wait()

    @pl.when(sub != root)
    def _():
        for s in range(subs):

            @pl.when(sub == s)
            def _():
                child_copy(s).wait_send()
                for b in range(s * per_sub, (s + 1) * per_sub):
                    row_copy_out(b).wait_recv()

        pltpu.make_async_copy(pairs, pairs, send_sem).wait()

    for b in range(blocks):
        if b:

            @pl.when(sub == b // per_sub)
            def _():
                fill(b).wait()


def merge(rows, dest, child, columns, damping, fronts, subs):
    rows_held, width = rows.shape
    size = 2 * width // LANES
    kids, _, contrib = child.shape
    groups = GROUPS
    deep = max(kids * contrib, 2 * fronts * subs // groups)
    blocks = width // BLOCK
    vmem = pl.BlockSpec(memory_space=pltpu.VMEM)
    return pl.pallas_call(
        lambda *refs: merge_kernel(fronts, subs, *refs),
        out_shape=jax.ShapeDtypeStruct((width // subs, width), F32),
        in_specs=[vmem, vmem, pl.BlockSpec(memory_space=pl.ANY), vmem, vmem],
        out_specs=pl.BlockSpec(memory_space=pl.ANY),
        scratch_shapes=[
            pltpu.VMEM((fronts * size, LANES), F32),
            pltpu.VMEM((fronts // 2, size, LANES), F32),
            pltpu.VMEM((fronts // 2, 2 * size, LANES), F32),
            pltpu.VMEM((fronts * subs * size, LANES), F32),
            pltpu.VMEM((subs,) + child.shape, F32),
            pltpu.VMEM((BLOCK, width), F32),
            pltpu.VMEM((deep, width), BF16),
            pltpu.VMEM((deep, width), BF16),
            pltpu.VMEM((width, width), F32),
            pltpu.VMEM((width, width), F32),
            pltpu.VMEM((width, width), BF16),
            pltpu.VMEM((width, width), BF16),
            pltpu.VMEM((BLOCK, BLOCK), F32),
            pltpu.VMEM((BLOCK, BLOCK), F32),
            pltpu.VMEM((BLOCK, BLOCK), F32),
            pltpu.SemaphoreType.DMA,
            pltpu.SemaphoreType.DMA,
            pltpu.SemaphoreType.DMA,
            pltpu.SemaphoreType.DMA((groups,)),
            pltpu.SemaphoreType.DMA,
            pltpu.SemaphoreType.DMA((subs,)),
            pltpu.SemaphoreType.DMA,
            pltpu.SemaphoreType.DMA((blocks // subs,)),
            pltpu.SemaphoreType.DMA((blocks,)),
            pltpu.SemaphoreType.DMA((blocks // subs,)),
        ],
        compiler_params=pltpu.CompilerParams(has_side_effects=True),
        name="front_merge",
    )(rows, dest, child, columns, damping)


def local(row_values, front_of_row, child_factors, child_columns, damping):
    fronts = lax.axis_size("front")
    subs = lax.axis_size("sub")
    return merge(row_values, front_of_row, child_factors, child_columns, damping, fronts, subs)[None]


def solution(mesh):
    in_specs = (
        P(("front", "sub"), None),
        P(("front", "sub"), None),
        P("front", "sub", None),
        P("front", None),
        P("front", None),
    )
    out_specs = P("front", "sub", None)
    return jax.shard_map(local, mesh=mesh, in_specs=in_specs, out_specs=out_specs, check_vma=False)
```

```python
import jax
import jax.numpy as jnp
from jax import lax
from jax.experimental import pallas as pl
from jax.experimental.pallas import tpu as pltpu
from jax.sharding import PartitionSpec as P

F32 = jnp.float32
BF16 = jnp.bfloat16
BLOCK = 128
LANES = 128
GROUP = 8
GROUPS = 4
STRIDE = 53
CUTS = (0, 4, 8)
MESH = pl.DeviceIdType.MESH
KEEP = (((1,), (0,)), ((), ()))
ROWS = (((0,), (0,)), ((), ()))
COLS = (((1,), (1,)), ((), ()))


def mm(left, right, dims):
    return lax.dot_general(left, right, dims, preferred_element_type=F32)


def split(x):
    high = x.astype(BF16)
    return high, (x - high.astype(F32)).astype(BF16)


def mm3(left, right, dims):
    return mm(left[0], right[0], dims) + (mm(left[0], right[1], dims) + mm(left[1], right[0], dims))


def root_of(front):
    return lax.rem(2 * (front % 2) + (front // 2) % 2 + front // 4 + front // 16, 4)


def lane_copy(x, j):
    return jnp.broadcast_to(x[:, j : j + 1], (GROUP, LANES))


def row_copy(x, j):
    return jnp.broadcast_to(x[j : j + 1, :], (GROUP, LANES))


def factor_block(source, upper_ref, inverse_ref):
    count = BLOCK // GROUP
    sub = lax.broadcasted_iota(jnp.int32, (GROUP, LANES), 0)
    lane = lax.broadcasted_iota(jnp.int32, (GROUP, LANES), 1)
    a = [source[GROUP * k : GROUP * (k + 1), :] for k in range(count)]
    e = [jnp.where(lane == sub + GROUP * k, 1.0, 0.0).astype(F32) for k in range(count)]
    zero = 0.0 * a[0]
    for k in range(count):
        b = [lane_copy(a[k], GROUP * k + m) + zero for m in range(GROUP)]
        more = k + 1 < count
        c = [lane_copy(a[k + 1], GROUP * k + m) for m in range(GROUP)] if more else None
        pivots = None
        for j in range(GROUP):
            pivot = row_copy(b[j], j)
            pivots = pivot if pivots is None else jnp.where(sub >= j, pivot, pivots)
            inv = 1.0 / pivot
            ratio = jnp.where(sub > j, b[j], 0.0) * inv
            below = c[j] * inv if more else None
            for m in range(j + 1, GROUP):
                u = row_copy(b[m], j)
                b[m] = b[m] - ratio * u
                if more:
                    c[m] = c[m] - below * u
            row_a, row_e = row_copy(a[k], j), row_copy(e[k], j)
            a[k] = a[k] - ratio * row_a
            e[k] = e[k] - ratio * row_e
            if more:
                a[k + 1] = a[k + 1] - below * row_a
                e[k + 1] = e[k + 1] - below * row_e
        scale = lax.rsqrt(pivots)
        top, side = a[k] * scale, e[k] * scale
        upper_ref[GROUP * k : GROUP * (k + 1), :] = top
        inverse_ref[GROUP * k : GROUP * (k + 1), :] = side
        if k + 2 < count:
            both = jnp.concatenate([top, side], axis=1)
            high = both.astype(BF16).astype(F32)
            low = both - high
            change = mm3((high[:, :LANES], low[:, :LANES]), (high, low), ROWS)
            for q in range(k + 2, count):
                a[q] = a[q] - change[GROUP * q : GROUP * (q + 1), :LANES]
                e[q] = e[q] - change[GROUP * q : GROUP * (q + 1), LANES:]


def merge_kernel(
    fronts,
    subs,
    rows_ref,
    dest_ref,
    child_ref,
    columns_ref,
    damping_ref,
    out_ref,
    slots,
    away,
    pairs,
    recv,
    children,
    zeros,
    kh,
    kl,
    xh,
    xl,
    gram,
    r_full,
    rh,
    rl,
    lh,
    ll,
    block,
    upper,
    inverse,
    pair_send,
    pair_recv,
    send_sem,
    recv_sem,
    child_send,
    child_recv,
    child_own,
    fill_sem,
    row_send,
    row_recv,
):
    me = lax.axis_index("front")
    sub = lax.axis_index("sub")
    root = root_of(me)
    rows_held, width = rows_ref.shape
    kids, _, contrib = child_ref.shape
    groups = recv_sem.shape[1]
    blocks = width // BLOCK
    per_sub = blocks // subs
    parts = len(CUTS) - 1
    wide = CUTS[1] - CUTS[0]
    size = 2 * wide

    def child_copy(s):
        return pltpu.make_async_remote_copy(
            src_ref=child_ref.at[:, :, s * BLOCK :],
            dst_ref=children.at[s, :, :, s * BLOCK :],
            send_sem=child_send,
            recv_sem=child_recv.at[s],
            device_id=(me, root),
            device_id_type=MESH,
        )

    def child_keep(s):
        return pltpu.make_async_copy(child_ref.at[:, :, s * BLOCK :], children.at[s, :, :, s * BLOCK :], child_own)

    for s in range(subs):

        @pl.when((sub == s) & (root != s))
        def _():
            child_copy(s).start()

        @pl.when((sub == s) & (root == s))
        def _():
            child_keep(s).start()

    def fill(b):
        half = b % per_sub
        return pltpu.make_async_copy(
            zeros.at[:, : b * BLOCK], out_ref.at[half * BLOCK : (half + 1) * BLOCK, : b * BLOCK], fill_sem.at[half]
        )

    zeros[...] = jnp.zeros_like(zeros)

    core = lax.rem(me, 2)
    pair = me // 2
    half = fronts // 2
    place = lax.broadcasted_iota(jnp.int32, (rows_held, fronts), 1)
    late = place >= half
    name = jnp.where(late, 2 * (place - half) + (1 - core), 2 * place + core)
    chosen = (dest_ref[...] == name).astype(F32)
    before = (
        lax.broadcasted_iota(jnp.int32, (rows_held, rows_held), 1)
        < lax.broadcasted_iota(jnp.int32, (rows_held, rows_held), 0)
    ).astype(BF16)
    earlier = mm(before, chosen.astype(BF16), KEEP)
    pieces = split(rows_ref[...])
    for slot in range(2):
        pick = jnp.where(earlier == slot, chosen, 0.0).astype(BF16)
        placed = mm(pick, pieces[0], ROWS) + mm(pick, pieces[1], ROWS)
        for p in range(parts):
            for k in range(wide):
                at = (CUTS[p] + k) * LANES
                slots[pl.ds(p * fronts * size + slot * wide + k, fronts, stride=size), :] = placed[:, at : at + LANES]
    for p in range(parts):
        for j in range(half):
            at = (p * fronts + j) * size
            pairs[p, j, :size, :] = slots[at : at + size, :]
            away[p, j] = slots[at + half * size : at + (half + 1) * size, :]

    def swap(p):
        return pltpu.make_async_remote_copy(
            src_ref=away.at[p],
            dst_ref=pairs.at[p, :, size:, :],
            send_sem=pair_send.at[p],
            recv_sem=pair_recv.at[p],
            device_id=(me + 1 - 2 * core, sub),
            device_id_type=MESH,
        )

    for p in range(parts):
        swap(p).start()
    steps = half // groups
    for p in range(parts):
        swap(p).wait()
        for g in range(groups):

            def send(i, carry):
                to = lax.rem(pair + STRIDE * i, half)
                front = 2 * to + core
                target = root_of(front)

                @pl.when((front != me) | (target != sub))
                def _():
                    pltpu.make_async_remote_copy(
                        src_ref=pairs.at[p, to],
                        dst_ref=recv.at[
                            pl.ds(pl.multiple_of(((p * half + i) * subs + sub) * 2 * size, 2 * size), 2 * size), :
                        ],
                        send_sem=send_sem.at[p],
                        recv_sem=recv_sem.at[p, g],
                        device_id=(front, target),
                        device_id_type=MESH,
                    ).start()

                return carry

            lax.fori_loop(g * steps, (g + 1) * steps, send, 0)

    for b in range(blocks):
        if b:

            @pl.when(sub == b // per_sub)
            def _():
                fill(b).start()

    def part_of(b):
        return [p for p in range(parts) if CUTS[p + 1] > b]

    def row_piece(b, p):
        half = b % per_sub
        lo, hi = max(b, CUTS[p]) * BLOCK, CUTS[p + 1] * BLOCK
        return r_full.at[b * BLOCK : (b + 1) * BLOCK, lo:hi], out_ref.at[half * BLOCK : (half + 1) * BLOCK, lo:hi]

    def row_copy_out(b, p):
        src, dst = row_piece(b, p)
        return pltpu.make_async_remote_copy(
            src_ref=src,
            dst_ref=dst,
            send_sem=row_send.at[b, p],
            recv_sem=row_recv.at[b % per_sub, p],
            device_id=(me, b // per_sub),
            device_id_type=MESH,
        )

    def row_keep(b, p):
        src, dst = row_piece(b, p)
        return pltpu.make_async_copy(src, dst, row_send.at[b, p])

    def row_out(b, p):
        @pl.when(root != b // per_sub)
        def _():
            row_copy_out(b, p).start()

        @pl.when(root == b // per_sub)
        def _():
            row_keep(b, p).start()

    @pl.when(sub == root)
    def _():
        for p in range(parts):
            recv[pl.ds(pl.multiple_of((p * half * subs + sub) * 2 * size, 2 * size), 2 * size), :] = pairs[p, pair]
        for s in range(subs):

            @pl.when(root == s)
            def _():
                child_keep(s).wait()

            @pl.when(root != s)
            def _():
                child_copy(s).wait_recv()

        for c in range(kids):
            spread = (
                lax.broadcasted_iota(jnp.int32, (width, contrib), 0) == columns_ref[c : c + 1, :]
            ).astype(F32).astype(BF16)
            for s in range(subs):
                high, low = split(children[s, c, :, s * BLOCK :])
                at = c * contrib + s * BLOCK
                kh[at : at + BLOCK, :] = mm(high, spread[:, s * BLOCK :], COLS).astype(BF16)
                kl[at : at + BLOCK, :] = mm(low, spread[:, s * BLOCK :], COLS).astype(BF16)
        on_diagonal = lax.broadcasted_iota(jnp.int32, (BLOCK, BLOCK), 0) == lax.broadcasted_iota(
            jnp.int32, (BLOCK, BLOCK), 1
        )
        count = 4 * steps * subs

        def columns_in(p):
            end = CUTS[p + 1] * BLOCK
            for b in range(CUTS[p + 1]):
                c0, c1 = b * BLOCK, (b + 1) * BLOCK
                lo = max(b, CUTS[p]) * BLOCK
                gram[c0:c1, lo:end] = mm3((kh[:, c0:c1], kl[:, c0:c1]), (kh[:, lo:end], kl[:, lo:end]), ROWS)
                if b >= CUTS[p]:
                    weight = damping_ref[:, c0:c1]
                    gram[c0:c1, c0:c1] += jnp.where(on_diagonal, weight * weight, 0.0)

            def gather(g, carry):
                for h in range(groups):

                    @pl.when(g == h)
                    def _():
                        first = 1 if h == 0 else 0
                        region = recv.at[pl.ds(0, (steps * subs - first) * 2 * size), :]
                        pltpu.make_async_copy(region, region, recv_sem.at[p, h]).wait()

                for q in range(count // BLOCK):
                    base = pl.multiple_of(g * count + q * BLOCK, BLOCK)
                    first = p * half * subs * 2 * size
                    for k in range(wide):
                        at = (CUTS[p] + k) * LANES
                        high, low = split(recv[pl.ds(first + base * wide + k, BLOCK, stride=wide), :])
                        xh[pl.ds(base, BLOCK), at : at + LANES] = high
                        xl[pl.ds(base, BLOCK), at : at + LANES] = low
                here = pl.ds(pl.multiple_of(g * count, count), count)
                for b in range(CUTS[p + 1]):
                    c0, c1 = b * BLOCK, (b + 1) * BLOCK
                    lo = max(b, CUTS[p]) * BLOCK
                    gram[c0:c1, lo:end] += mm3(
                        (xh[here, c0:c1], xl[here, c0:c1]), (xh[here, lo:end], xl[here, lo:end]), ROWS
                    )
                return carry

            lax.fori_loop(0, groups, gather, 0)

        def finish(b, lo, hi, inverse_parts):
            c0, c1 = b * BLOCK, (b + 1) * BLOCK
            rest = mm3(inverse_parts, split(gram[c0:c1, lo:hi]), KEEP)
            r_full[c0:c1, lo:hi] = rest
            rh[c0:c1, lo:hi], rl[c0:c1, lo:hi] = split(rest)

        def reduce(b, lo, hi):
            c0, c1 = b * BLOCK, (b + 1) * BLOCK
            gram[c0:c1, lo:hi] -= mm3((rh[:c0, c0:c1], rl[:c0, c0:c1]), (rh[:c0, lo:hi], rl[:c0, lo:hi]), ROWS)

        def step(i, carry):
            for p in range(parts):
                for b in range(CUTS[p], CUTS[p + 1]):

                    @pl.when(i == b)
                    def _():
                        lo, hi = CUTS[p] * BLOCK, CUTS[p + 1] * BLOCK
                        c0, c1 = b * BLOCK, (b + 1) * BLOCK
                        if b == CUTS[p]:
                            columns_in(p)
                            for q in range(b):
                                if q:
                                    reduce(q, lo, hi)
                                at = slice(q * BLOCK, (q + 1) * BLOCK)
                                finish(q, lo, hi, (lh[at, :], ll[at, :]))
                                row_out(q, p)
                        if b:
                            reduce(b, c0, hi)
                        block[...] = gram[c0:c1, c0:c1]

            factor_block(block, upper, inverse)
            for p in range(parts):
                for b in range(CUTS[p], CUTS[p + 1]):

                    @pl.when(i == b)
                    def _():
                        hi = CUTS[p + 1] * BLOCK
                        c0, c1 = b * BLOCK, (b + 1) * BLOCK
                        r_full[c0:c1, c0:c1] = upper[...]
                        solve = split(inverse[...])
                        if p + 1 < parts:
                            lh[c0:c1, :], ll[c0:c1, :] = solve
                        if c1 < hi:
                            finish(b, c1, hi, solve)
                        row_out(b, p)

            return carry

        lax.fori_loop(0, blocks, step, 0)
        for b in range(blocks):
            for p in part_of(b):

                @pl.when(root != b // per_sub)
                def _():
                    row_copy_out(b, p).wait_send()

                @pl.when(root == b // per_sub)
                def _():
                    row_keep(b, p).wait()

        for p in range(parts):
            sent = pairs.at[p, pl.ds(0, half - 1)]
            pltpu.make_async_copy(sent, sent, send_sem.at[p]).wait()

    @pl.when(sub != root)
    def _():
        for s in range(subs):

            @pl.when(sub == s)
            def _():
                child_copy(s).wait_send()
                for b in range(s * per_sub, (s + 1) * per_sub):
                    for p in part_of(b):
                        row_copy_out(b, p).wait_recv()

        for p in range(parts):
            pltpu.make_async_copy(pairs.at[p], pairs.at[p], send_sem.at[p]).wait()

    for b in range(blocks):
        if b:

            @pl.when(sub == b // per_sub)
            def _():
                fill(b).wait()


def merge(rows, dest, child, columns, damping, fronts, subs):
    rows_held, width = rows.shape
    parts = len(CUTS) - 1
    size = 2 * (CUTS[1] - CUTS[0])
    kids, _, contrib = child.shape
    blocks = width // BLOCK
    half = fronts // 2
    solved = CUTS[-2] * BLOCK
    vmem = pl.BlockSpec(memory_space=pltpu.VMEM)
    return pl.pallas_call(
        lambda *refs: merge_kernel(fronts, subs, *refs),
        out_shape=jax.ShapeDtypeStruct((width // subs, width), F32),
        in_specs=[vmem, vmem, pl.BlockSpec(memory_space=pl.ANY), vmem, vmem],
        out_specs=pl.BlockSpec(memory_space=pl.ANY),
        scratch_shapes=[
            pltpu.VMEM((parts * fronts * size, LANES), F32),
            pltpu.VMEM((parts, half, size, LANES), F32),
            pltpu.VMEM((parts, half, 2 * size, LANES), F32),
            pltpu.VMEM((parts * half * subs * 2 * size, LANES), F32),
            pltpu.VMEM((subs,) + child.shape, F32),
            pltpu.VMEM((BLOCK, width), F32),
            pltpu.VMEM((kids * contrib, width), BF16),
            pltpu.VMEM((kids * contrib, width), BF16),
            pltpu.VMEM((2 * fronts * subs, width), BF16),
            pltpu.VMEM((2 * fronts * subs, width), BF16),
            pltpu.VMEM((width, width), F32),
            pltpu.VMEM((width, width), F32),
            pltpu.VMEM((width, width), BF16),
            pltpu.VMEM((width, width), BF16),
            pltpu.VMEM((solved, BLOCK), BF16),
            pltpu.VMEM((solved, BLOCK), BF16),
            pltpu.VMEM((BLOCK, BLOCK), F32),
            pltpu.VMEM((BLOCK, BLOCK), F32),
            pltpu.VMEM((BLOCK, BLOCK), F32),
            pltpu.SemaphoreType.DMA((parts,)),
            pltpu.SemaphoreType.DMA((parts,)),
            pltpu.SemaphoreType.DMA((parts,)),
            pltpu.SemaphoreType.DMA((parts, GROUPS)),
            pltpu.SemaphoreType.DMA,
            pltpu.SemaphoreType.DMA((subs,)),
            pltpu.SemaphoreType.DMA,
            pltpu.SemaphoreType.DMA((blocks // subs,)),
            pltpu.SemaphoreType.DMA((blocks, parts)),
            pltpu.SemaphoreType.DMA((blocks // subs, parts)),
        ],
        compiler_params=pltpu.CompilerParams(has_side_effects=True),
        name="front_merge",
    )(rows, dest, child, columns, damping)


def local(row_values, front_of_row, child_factors, child_columns, damping):
    fronts = lax.axis_size("front")
    subs = lax.axis_size("sub")
    return merge(row_values, front_of_row, child_factors, child_columns, damping, fronts, subs)[None]


def solution(mesh):
    in_specs = (
        P(("front", "sub"), None),
        P(("front", "sub"), None),
        P("front", "sub", None),
        P("front", None),
        P("front", None),
    )
    out_specs = P("front", "sub", None)
    return jax.shard_map(local, mesh=mesh, in_specs=in_specs, out_specs=out_specs, check_vma=False)
```
